256 devices in a mesh: band: 8 (over z_hi, y), grid: 32 (over z_lo, x, core).
Axes of the slice: x: 4, y: 4, z: 8 (z_hi: 2, z_lo: 4; z = z_hi * 4 + z_lo), core: 2. Of those that a mesh axis runs over, the one named last changes fastest.
Arguments:
- orbitals: bfloat16 [2048, 65536], P('band', 'grid'), as said below
- projectors: bfloat16 [2048, 65536], P('band', 'grid'), may hold values from -0.015625 to 0.015625
Outputs:
- result: bfloat16 [2048, 65536], P('band', 'grid')
- energies: float32 [2048], P('band')
The draws below stay inside these ranges and needn't reach their ends.
Inputs may be any that keep to these rules, and one draw needn't show every extreme that they name: The orbitals are real-valued.
All inputs are finite; a program needn't handle non-finite values.
Results may differ from the reference program's by a relative error of at most 0.0049.
Values may be sent and summed in bfloat16 or wider, within the bound.
No kernel may reach another device: no remote copies, remote signals or barrier semaphores. Data moves between devices by JAX's collectives and lax.ppermute only.
A program may use at most 64 MiB of HBM per device.

```python
import jax
import jax.numpy as jnp
from jax import lax

NB = 2048
NG = 65536


def draw_orbitals(key, part):
    k_main = jax.random.fold_in(key, 11)
    k_rough = jax.random.fold_in(key, 12)
    place = jnp.arange(NG, dtype=jnp.float32) / (NG - 1)
    rising = 0.6 + 1.2 * place
    rough = jax.random.uniform(k_rough, (1, NG), jnp.float32, 0.5, 1.5)
    values = jax.random.normal(k_main, (NB, NG), jnp.float32)
    return (values * rising[None, :] * rough).astype(jnp.bfloat16)


def steps_of(rng, shape, pieces, smallest, top_value):
    factor_of = 1.0
    for dim, shards_of in pieces:
        steps = jax.random.uniform(jax.random.fold_in(jax.random.fold_in(rng, 6), dim), (shards_of,), jnp.float32, smallest / len(pieces), top_value / len(pieces))
        factor_of = factor_of * jnp.repeat(jnp.exp(steps), shape[dim] // shards_of).reshape((-1,) + (1,) * (len(shape) - 1 - dim))
    return factor_of


def normal_values(rng, dims, scale, limit, shards=(), kind=jnp.bfloat16):
    array = jax.random.normal(rng, dims, jnp.float32) * scale
    if len(shards) > 0:
        array = steps_of(rng, dims, shards, -0.22, 0.18) * array
    return jnp.clip(array, min=-limit, max=limit).astype(kind)


def setup_inputs(seed: int = 0) -> dict:
    splits = jax.random.split(jax.random.key(seed), 3)
    return {
        "orbitals": draw_orbitals(jax.random.fold_in(splits[2], 71), 0),
        "projectors": normal_values(splits[1], (NB, NG), (2 * NG) ** -0.5, 0.015625, ((0, 8), (1, 32))),
    }


def intersections(projectors, state):
    return jnp.dot(projectors.astype(jnp.float32), state.astype(jnp.float32).T, preferred_element_type=jnp.float32)


def update(projectors, state, rounded):
    widened = lax.optimization_barrier(rounded).astype(jnp.float32)
    return state.astype(jnp.float32) - jnp.dot(widened.T, projectors.astype(jnp.float32), preferred_element_type=jnp.float32)


def reference(orbitals, projectors):
    first = intersections(projectors, orbitals)
    first_b = first.astype(jnp.bfloat16)
    middle = update(projectors, orbitals, first_b).astype(jnp.bfloat16)
    second = intersections(projectors, middle)
    second_b = second.astype(jnp.bfloat16)
    result = update(projectors, middle, second_b).astype(jnp.bfloat16)
    wide = middle.astype(jnp.float32)
    norm = jnp.sum(wide * wide, axis=1)
    numer = jnp.sum(second * lax.optimization_barrier(second_b).astype(jnp.float32), axis=0)
    energies = (2.0 * NG / NB) * numer / norm
    return result, energies
```

```python
import jax
import jax.numpy as jnp
from jax import lax
from jax.sharding import PartitionSpec as P


ZL, NX, NC = 4, 4, 2
ZH, NY = 2, 4


def fetch_band(array, dz, dy):
    pairs = [
        (((z + dz) % ZH) * NY + (y + dy) % NY, z * NY + y)
        for z in range(ZH)
        for y in range(NY)
    ]
    return lax.ppermute(array, "band", pairs)


def grid_pairs(source):
    return [
        (source(zl, x, c), zl * 8 + x * 2 + c)
        for zl in range(ZL)
        for x in range(NX)
        for c in range(NC)
    ]


def from_core(array):
    return lax.ppermute(array, "grid", grid_pairs(lambda zl, x, c: zl * 8 + x * 2 + 1 - c))


def from_x(array, d):
    return lax.ppermute(
        array, "grid", grid_pairs(lambda zl, x, c: zl * 8 + ((x + d) % NX) * 2 + c)
    )


def from_zl(array, d):
    return lax.ppermute(array, "grid", grid_pairs(lambda zl, x, c: (zl ^ d) * 8 + x * 2 + c))


def position():
    g = lax.axis_index("grid")
    return g // 8, (g // 2) % 4, g % 2


def pick(array, at, axis):
    return lax.dynamic_index_in_dim(array, at, axis, keepdims=False)


def reduce_over_grid(partial):
    zl, x, c = position()
    n, _, cols = partial.shape
    parts = partial.reshape(n, NC, NX, ZL, 8, cols)
    there = from_core(pick(parts, 1 - c, 1).astype(jnp.bfloat16))
    parts = pick(parts, c, 1) + there.astype(jnp.float32)
    total = pick(parts, x, 1)
    for d in (1, 3, 2):
        there = from_x(pick(parts, (x + NX - d) % NX, 1).astype(jnp.bfloat16), d)
        total = total + there.astype(jnp.float32)
    parts = total
    total = pick(parts, zl, 1)
    for d in (1, 2, 3):
        there = from_zl(pick(parts, zl ^ d, 1).astype(jnp.bfloat16), d)
        total = total + there.astype(jnp.float32)
    return total


def placed(pieces, axis):
    length = len(pieces)
    shape = list(pieces[0][1].shape)
    shape.insert(axis, length)
    out = jnp.zeros(shape, pieces[0][1].dtype)
    for at, piece in pieces:
        out = lax.dynamic_update_index_in_dim(out, piece, at, axis)
    return out


def gather_over_grid(rows):
    zl, x, c = position()
    held = placed([(zl, rows)] + [(zl ^ d, from_zl(rows, d)) for d in (1, 2, 3)], 1)
    held = placed([(x, held)] + [((x + d) % NX, from_x(held, d)) for d in (1, 3, 2)], 1)
    return placed([(c, held), (1 - c, from_core(held))], 1)


def intersect(rows, state):
    return lax.dot_general(
        rows, state, (((1,), (1,)), ((), ())), preferred_element_type=jnp.float32
    )


def apply(rounded, rows):
    return lax.dot_general(
        rounded, rows, (((0,), (0,)), ((), ())), preferred_element_type=jnp.float32
    )


def halves(value):
    high = lax.reduce_precision(value, 8, 7)
    return high.astype(jnp.bfloat16), (value - high).astype(jnp.bfloat16)


def gather_projectors(projectors):
    got = {}
    got["00a"], got["00b"] = projectors[:128], projectors[128:]
    got["01a"] = fetch_band(got["00a"], 0, 1)
    got["03b"] = fetch_band(got["00b"], 0, 3)
    got["10a"] = fetch_band(got["00a"], 1, 0)
    got["01b"] = fetch_band(got["00b"], 0, 1)
    got["03a"] = fetch_band(got["00a"], 0, 3)
    got["10b"] = fetch_band(got["00b"], 1, 0)
    got["02a"] = fetch_band(got["01a"], 0, 1)
    got["02b"] = fetch_band(got["03b"], 0, 3)
    got["11a"] = fetch_band(got["10a"], 0, 1)
    got["13a"] = fetch_band(got["10a"], 0, 3)
    got["13b"] = fetch_band(got["10b"], 0, 3)
    got["12a"] = fetch_band(got["11a"], 0, 1)
    got["11b"] = fetch_band(got["10b"], 0, 1)
    got["12b"] = fetch_band(got["13b"], 0, 3)
    return got


GROUPS = (("00", "01", "03"), ("02", "10"), ("11", "13", "12"))


def per_device(orbitals, projectors):
    total_bands = projectors.shape[0] * lax.axis_size("band")
    total_points = projectors.shape[1] * lax.axis_size("grid")
    got = gather_projectors(projectors)

    shares = []
    for group in GROUPS:
        terms = [intersect(got[k + h], orbitals) for k in group for h in "ab"]
        shares.append(reduce_over_grid(jnp.stack(terms).reshape(len(group), 256, 256)))
    share_b = jnp.concatenate(shares).astype(jnp.bfloat16)
    first_b = gather_over_grid(share_b).reshape(-1, 256)
    whole = jnp.concatenate([got[k + h] for group in GROUPS for k in group for h in "ab"])
    middle = (orbitals.astype(jnp.float32) - apply(first_b, whole)).astype(jnp.bfloat16)
    widened = middle.astype(jnp.float32)
    norm = jnp.sum(widened * widened, axis=1)

    terms = intersect(whole, middle)
    share = reduce_over_grid(terms.reshape(8, 256, 256))
    share_b = share.astype(jnp.bfloat16)
    value = jnp.sum(share * share_b.astype(jnp.float32), axis=(0, 1))
    sums = jnp.stack([*halves(value), *halves(norm)])
    sums = jnp.concatenate([sums, jnp.zeros((4, 256), jnp.bfloat16)])
    gathered = gather_over_grid(jnp.concatenate([share_b, sums[None]]))
    second_b = gathered[:8].reshape(-1, 256)
    sums = jnp.sum(gathered[8, ..., :4, :].astype(jnp.float32), axis=(0, 1, 2))
    result = (widened - apply(second_b, whole)).astype(jnp.bfloat16)
    energies = 2.0 * total_points / total_bands * (sums[0] + sums[1]) / (sums[2] + sums[3])
    return (result, energies)


def solution(mesh):
    in_specs = (P("band", "grid"), P("band", "grid"))
    out_specs = (P("band", "grid"), P("band"))
    return jax.shard_map(
        per_device, mesh=mesh, in_specs=in_specs, out_specs=out_specs, check_vma=False
    )
```

```python
import jax
import jax.numpy as jnp
from jax import lax
from jax.sharding import PartitionSpec as P


ZL, NX, NC = 4, 4, 2
ZH, NY = 2, 4


def fetch_band(array, dz, dy):
    pairs = [
        (((z + dz) % ZH) * NY + (y + dy) % NY, z * NY + y)
        for z in range(ZH)
        for y in range(NY)
    ]
    return lax.ppermute(array, "band", pairs)


def grid_pairs(source):
    return [
        (source(zl, x, c), zl * 8 + x * 2 + c)
        for zl in range(ZL)
        for x in range(NX)
        for c in range(NC)
    ]


def from_core(array):
    return lax.ppermute(array, "grid", grid_pairs(lambda zl, x, c: zl * 8 + x * 2 + 1 - c))


def from_x(array, d):
    return lax.ppermute(
        array, "grid", grid_pairs(lambda zl, x, c: zl * 8 + ((x + d) % NX) * 2 + c)
    )


def from_zl(array, d):
    return lax.ppermute(array, "grid", grid_pairs(lambda zl, x, c: (zl ^ d) * 8 + x * 2 + c))


def position():
    g = lax.axis_index("grid")
    return g // 8, (g // 2) % 4, g % 2


def pick(array, at, axis):
    return lax.dynamic_index_in_dim(array, at, axis, keepdims=False)


def reduce_over_grid(partial):
    zl, x, c = position()
    n, _, cols = partial.shape
    parts = partial.reshape(n, NC, NX, ZL, 8, cols)
    there = from_core(pick(parts, 1 - c, 1).astype(jnp.bfloat16))
    parts = pick(parts, c, 1) + there.astype(jnp.float32)
    total = pick(parts, x, 1)
    for d in (1, 3, 2):
        there = from_x(pick(parts, (x + NX - d) % NX, 1).astype(jnp.bfloat16), d)
        total = total + there.astype(jnp.float32)
    parts = total
    total = pick(parts, zl, 1)
    for d in (1, 2, 3):
        there = from_zl(pick(parts, zl ^ d, 1).astype(jnp.bfloat16), d)
        total = total + there.astype(jnp.float32)
    return total


def placed(pieces, axis):
    length = len(pieces)
    shape = list(pieces[0][1].shape)
    shape.insert(axis, length)
    out = jnp.zeros(shape, pieces[0][1].dtype)
    for at, piece in pieces:
        out = lax.dynamic_update_index_in_dim(out, piece, at, axis)
    return out


def gather_over_grid(rows):
    zl, x, c = position()
    held = placed([(zl, rows)] + [(zl ^ d, from_zl(rows, d)) for d in (1, 2, 3)], 1)
    held = placed([(x, held)] + [((x + d) % NX, from_x(held, d)) for d in (1, 3, 2)], 1)
    return placed([(c, held), (1 - c, from_core(held))], 1)


def intersect(rows, state):
    return lax.dot_general(
        rows, state, (((1,), (1,)), ((), ())), preferred_element_type=jnp.float32
    )


def apply(rounded, rows):
    return lax.dot_general(
        rounded, rows, (((0,), (0,)), ((), ())), preferred_element_type=jnp.float32
    )


def halves(value):
    high = lax.reduce_precision(value, 8, 7)
    return high.astype(jnp.bfloat16), (value - high).astype(jnp.bfloat16)


def gather_projectors(mine):
    got = {(0, 0): [mine]}
    upper = fetch_band(mine, 0, 1)
    lower = fetch_band(mine, 0, 3)
    first = fetch_band(mine[:128], 1, 0)
    second = fetch_band(mine[128:], 1, 0)
    got[0, 1], got[0, 3] = [upper], [lower]
    got[0, 2] = [fetch_band(upper[:128], 0, 1), fetch_band(lower[128:], 0, 3)]
    got[1, 0] = [first, second]
    got[1, 1] = [fetch_band(first, 0, 1)]
    got[1, 3] = [fetch_band(first, 0, 3)]
    got[1, 1] += [fetch_band(second, 0, 1)]
    got[1, 3] += [fetch_band(second, 0, 3)]
    got[1, 2] = [fetch_band(got[1, 1][0], 0, 1), fetch_band(got[1, 3][1], 0, 3)]
    return got


def gather_gram(rows):
    pair = jnp.stack([rows, fetch_band(rows, 1, 0)])
    return jnp.stack([pair] + [fetch_band(pair, 0, d) for d in (1, 2, 3)], axis=1)


def per_device(orbitals, projectors):
    total_bands = projectors.shape[0] * lax.axis_size("band")
    total_points = projectors.shape[1] * lax.axis_size("grid")
    got = gather_projectors(projectors)
    states = jnp.concatenate([orbitals, projectors])

    shares = []
    for z in range(ZH):
        terms = [intersect(rows, states) for y in range(NY) for rows in got[z, y]]
        terms = jnp.concatenate(terms).reshape(NY, 256, 512)
        shares.append(reduce_over_grid(terms))
    share = jnp.stack(shares)
    first, gram = share[..., :256], share[..., 256:]
    gram = gather_gram(jnp.stack(halves(gram), axis=2).reshape(ZH, NY, 16, 256))
    first_b = gather_over_grid(first.astype(jnp.bfloat16).reshape(8, 8, 256)).reshape(-1, 256)

    product = lax.dot_general(
        gram.reshape(8, 128, 256),
        first_b.reshape(8, 256, 256),
        (((2,), (1,)), ((0,), (0,))),
        preferred_element_type=jnp.float32,
    )
    product = product.reshape(ZH, NY, ZH, NY, 2, 8, 256).sum(axis=4)
    second = first
    for z in range(ZH):
        for y in range(NY):
            second = second - jnp.roll(product[z, y], (z, y), axis=(0, 1))

    second_b = second.astype(jnp.bfloat16)
    value = jnp.sum(second * second_b.astype(jnp.float32), axis=(0, 1, 2))

    whole = jnp.concatenate(
        [rows for z in range(ZH) for y in range(NY) for rows in got[z, y]]
    )
    middle = (orbitals.astype(jnp.float32) - apply(first_b, whole)).astype(jnp.bfloat16)
    widened = middle.astype(jnp.float32)
    norm = jnp.sum(widened * widened, axis=1)

    sums = jnp.stack([*halves(value), *halves(norm)])
    sums = jnp.concatenate([sums, jnp.zeros((4, 256), jnp.bfloat16)])
    gathered = gather_over_grid(jnp.concatenate([second_b.reshape(8, 8, 256), sums[None]]))
    second_b = gathered[:8].reshape(-1, 256)
    sums = jnp.sum(gathered[8, ..., :4, :].astype(jnp.float32), axis=(0, 1, 2))
    result = (widened - apply(second_b, whole)).astype(jnp.bfloat16)
    energies = 2.0 * total_points / total_bands * (sums[0] + sums[1]) / (sums[2] + sums[3])
    return (result, energies)


def solution(mesh):
    in_specs = (P("band", "grid"), P("band", "grid"))
    out_specs = (P("band", "grid"), P("band"))
    return jax.shard_map(
        per_device, mesh=mesh, in_specs=in_specs, out_specs=out_specs, check_vma=False
    )
```

```python
import jax
import jax.numpy as jnp
from jax import lax
from jax.sharding import PartitionSpec as P


ZL, NX, NC = 4, 4, 2
ZH, NY = 2, 4


def fetch_band(array, dz, dy):
    pairs = [
        (((z + dz) % ZH) * NY + (y + dy) % NY, z * NY + y)
        for z in range(ZH)
        for y in range(NY)
    ]
    return lax.ppermute(array, "band", pairs)


def grid_pairs(source):
    return [
        (source(zl, x, c), zl * 8 + x * 2 + c)
        for zl in range(ZL)
        for x in range(NX)
        for c in range(NC)
    ]


def from_core(array):
    return lax.ppermute(array, "grid", grid_pairs(lambda zl, x, c: zl * 8 + x * 2 + 1 - c))


def from_x(array, d):
    return lax.ppermute(
        array, "grid", grid_pairs(lambda zl, x, c: zl * 8 + ((x + d) % NX) * 2 + c)
    )


def from_zl(array, d):
    return lax.ppermute(array, "grid", grid_pairs(lambda zl, x, c: (zl ^ d) * 8 + x * 2 + c))


def position():
    g = lax.axis_index("grid")
    return g // 8, (g // 2) % 4, g % 2


def pick(array, at, axis):
    return lax.dynamic_index_in_dim(array, at, axis, keepdims=False)


def reduce_over_grid(mine, theirs):
    zl, x, _ = position()
    n, _, cols = mine.shape
    there = from_core(theirs.astype(jnp.bfloat16))
    parts = (mine + there.astype(jnp.float32)).reshape(n, NX, ZL, 8, cols)
    there = []
    for d in (1, 3, 2):
        part = pick(parts, (x + NX - d) % NX, 1).astype(jnp.bfloat16)
        there.append(from_x(part, d))
    parts = sum((t.astype(jnp.float32) for t in there), pick(parts, x, 1))
    there = []
    for d in (1, 2, 3):
        part = pick(parts, zl ^ d, 1).astype(jnp.bfloat16)
        there.append(from_zl(part, d))
    return sum((t.astype(jnp.float32) for t in there), pick(parts, zl, 1))


def placed(pieces, axis):
    length = len(pieces)
    shape = list(pieces[0][1].shape)
    shape.insert(axis, length)
    out = jnp.zeros(shape, pieces[0][1].dtype)
    for at, piece in pieces:
        out = lax.dynamic_update_index_in_dim(out, piece, at, axis)
    return out


def gather_over_grid(rows):
    zl, x, _ = position()
    there = [(zl ^ d, from_zl(rows, d)) for d in (1, 2, 3)]
    held = placed([(zl, rows)] + there, 1)
    there = [((x + d) % NX, from_x(held, d)) for d in (1, 3, 2)]
    held = placed([(x, held)] + there, 1)
    return held, from_core(held)


def intersect(rows, state):
    return lax.dot_general(
        rows, state, (((1,), (1,)), ((), ())), preferred_element_type=jnp.float32
    )


def apply(rounded, rows):
    return lax.dot_general(
        rounded, rows, (((0,), (0,)), ((), ())), preferred_element_type=jnp.float32
    )


def halves(value):
    high = lax.reduce_precision(value, 8, 7)
    return high.astype(jnp.bfloat16), (value - high).astype(jnp.bfloat16)


def gather_projectors(mine):
    up = fetch_band(mine, 0, 1)
    down = fetch_band(mine, 0, 3)
    up_up = fetch_band(up, 0, 1)
    plane = {0: mine, 1: up, 2: up_up, 3: down}
    beyond = []
    for half in range(2):
        rows = pick(mine.reshape(2, 128, -1), abs(half - position()[2]), 0)
        over = fetch_band(rows, 1, 0)
        up = fetch_band(over, 0, 1)
        down = fetch_band(over, 0, 3)
        beyond.append({0: over, 1: up, 2: fetch_band(down, 0, 3), 3: down})
    return plane, beyond


def gather_gram(rows):
    c = position()[2]
    pair = jnp.stack([rows, fetch_band(rows, 1, 0)])
    pairs = [pair] + [fetch_band(pair, 0, d) for d in (1, 2, 3)]
    near, far = [], []
    for z in range(ZH):
        for y in range(NY):
            block = jnp.roll(pairs[y][z], (z, y), axis=(0, 1))
            near.append(jnp.where(c == 0, block[..., :128], block[..., 128:]))
            far.append(jnp.where(c == 0, block[..., 128:], block[..., :128]))
    return [jnp.concatenate(h, axis=-1).reshape(64, 1024) for h in (near, far)]


ARRIVAL = (0, 1, 3, 2)


def by_core(blocks):
    c = position()[2]
    blocks = blocks.reshape(-1, 2, 128, blocks.shape[-1])
    return pick(blocks, c, 1), pick(blocks, 1 - c, 1)


def per_device(orbitals, projectors):
    total_bands = projectors.shape[0] * lax.axis_size("band")
    total_points = projectors.shape[1] * lax.axis_size("grid")
    square = jnp.sum(jnp.square(orbitals.astype(jnp.float32)), axis=1)
    plane, beyond = gather_projectors(projectors)

    states = jnp.concatenate([orbitals, projectors])
    terms = [intersect(plane[y], states) for y in ARRIVAL]
    here = reduce_over_grid(*by_core(jnp.concatenate(terms)))
    terms = [
        jnp.concatenate([intersect(beyond[half][y], states) for y in ARRIVAL])
        for half in range(2)
    ]
    there = reduce_over_grid(*(t.reshape(NY, 128, 512) for t in terms))
    sums = jnp.stack([s[ARRIVAL.index(y)] for s in (here, there) for y in range(NY)])
    first, gram = sums[..., :256], sums[..., 256:]
    gram_near, gram_far = gather_gram(gram.astype(jnp.bfloat16).reshape(ZH, NY, 8, 256))

    near, far = by_core(jnp.concatenate([plane[y] for y in range(NY)]))
    near = jnp.concatenate([near.reshape(512, -1)] + [beyond[0][y] for y in range(NY)])
    far = jnp.concatenate([far.reshape(512, -1)] + [beyond[1][y] for y in range(NY)])

    first_b = first.astype(jnp.bfloat16)
    mine, other = gather_over_grid(first_b)
    mine, other = mine.reshape(1024, 256), other.reshape(1024, 256)
    first, first_b = first.reshape(64, 256), first_b.reshape(64, 256)
    second = first - jnp.dot(gram_near, mine, preferred_element_type=jnp.float32)
    second = second - jnp.dot(gram_far, other, preferred_element_type=jnp.float32)
    second_b = second.astype(jnp.bfloat16)
    value = jnp.sum(second * second_b.astype(jnp.float32), axis=0)
    norm = square - jnp.sum(first_b.astype(jnp.float32) * (first + second), axis=0)

    middle = orbitals.astype(jnp.float32) - apply(mine, near)
    middle = (middle - apply(other, far)).astype(jnp.bfloat16)
    widened = middle.astype(jnp.float32)

    sums = jnp.stack([*halves(value), *halves(norm)])
    sums = jnp.concatenate([sums, jnp.zeros((4, 256), jnp.bfloat16)])
    rows = jnp.concatenate([second_b.reshape(8, 8, 256), sums[None]])
    mine, other = gather_over_grid(rows)
    sums = sum(h[8, ..., :4, :].astype(jnp.float32).sum(axis=(0, 1)) for h in (mine, other))
    result = widened - apply(mine[:8].reshape(1024, 256), near)
    result = (result - apply(other[:8].reshape(1024, 256), far)).astype(jnp.bfloat16)
    energies = 2.0 * total_points / total_bands * (sums[0] + sums[1]) / (sums[2] + sums[3])
    return (result, energies)


def solution(mesh):
    in_specs = (P("band", "grid"), P("band", "grid"))
    out_specs = (P("band", "grid"), P("band"))
    return jax.shard_map(
        per_device, mesh=mesh, in_specs=in_specs, out_specs=out_specs, check_vma=False
    )
```

```python
import jax
import jax.numpy as jnp
from jax import lax
from jax.sharding import PartitionSpec as P


ZL, NX, NC = 4, 4, 2
ZH, NY = 2, 4


def fetch_band(array, dz, dy):
    pairs = [
        (((z + dz) % ZH) * NY + (y + dy) % NY, z * NY + y)
        for z in range(ZH)
        for y in range(NY)
    ]
    return lax.ppermute(array, "band", pairs)


def grid_pairs(source):
    return [
        (source(zl, x, c), zl * 8 + x * 2 + c)
        for zl in range(ZL)
        for x in range(NX)
        for c in range(NC)
    ]


def from_core(array):
    return lax.ppermute(array, "grid", grid_pairs(lambda zl, x, c: zl * 8 + x * 2 + 1 - c))


def from_x(array, d):
    return lax.ppermute(
        array, "grid", grid_pairs(lambda zl, x, c: zl * 8 + ((x + d) % NX) * 2 + c)
    )


def from_zl(array, d):
    return lax.ppermute(array, "grid", grid_pairs(lambda zl, x, c: (zl ^ d) * 8 + x * 2 + c))


def position():
    g = lax.axis_index("grid")
    return g // 8, (g // 2) % 4, g % 2


def pick(array, at, axis):
    return lax.dynamic_index_in_dim(array, at, axis, keepdims=False)


def reduce_over_x(mine, theirs):
    x = position()[1]
    n, _, cols = mine.shape
    there = from_core(theirs.astype(jnp.bfloat16))
    parts = (mine + there.astype(jnp.float32)).reshape(n, NX, ZL, 8, cols)
    there = []
    for d in (1, 3, 2):
        part = pick(parts, (x + NX - d) % NX, 1).astype(jnp.bfloat16)
        there.append(from_x(part, d))
    return sum((t.astype(jnp.float32) for t in there), pick(parts, x, 1))


def reduce_over_zl(parts):
    zl = position()[0]
    parts = parts.reshape(parts.shape[0], 2, 2, 8, parts.shape[3])
    for d, bit in ((2, zl // 2), (1, zl % 2)):
        there = from_zl(pick(parts, 1 - bit, 1).astype(jnp.bfloat16), d)
        parts = pick(parts, bit, 1) + there.astype(jnp.float32)
    return parts


def placed(pieces, axis):
    length = len(pieces)
    shape = list(pieces[0][1].shape)
    shape.insert(axis, length)
    out = jnp.zeros(shape, pieces[0][1].dtype)
    for at, piece in pieces:
        out = lax.dynamic_update_index_in_dim(out, piece, at, axis)
    return out


def gather_over_grid(rows):
    zl, x, _ = position()
    there = from_zl(rows, 1)
    held = placed([(zl % 2, rows), (1 - zl % 2, there)], 1)
    there = from_zl(held, 2)
    held = placed([(zl // 2, held), (1 - zl // 2, there)], 1)
    held = held.reshape(held.shape[0], ZL, *held.shape[3:])
    there = [((x + d) % NX, from_x(held, d)) for d in (1, 3, 2)]
    held = placed([(x, held)] + there, 1)
    return held, from_core(held)


def intersect(rows, state):
    return lax.dot_general(
        rows, state, (((1,), (1,)), ((), ())), preferred_element_type=jnp.float32
    )


def apply(rounded, rows):
    return lax.dot_general(
        rounded, rows, (((0,), (0,)), ((), ())), preferred_element_type=jnp.float32
    )


def halves(value):
    high = lax.reduce_precision(value, 8, 7)
    return high.astype(jnp.bfloat16), (value - high).astype(jnp.bfloat16)


def gather_projectors(mine):
    up = fetch_band(mine, 0, 1)
    down = fetch_band(mine, 0, 3)
    over = fetch_band(mine, 1, 0)
    up_up = fetch_band(up, 0, 1)
    over_up = fetch_band(over, 0, 1)
    over_down = fetch_band(over, 0, 3)
    last = [fetch_band(over_up[:128], 0, 1), fetch_band(over_down[128:], 0, 3)]
    last = jnp.concatenate(last)
    return [[mine], [up], [up_up], [down]], [[over], [over_up], [last], [over_down]]


def gather_gram(rows):
    c = position()[2]
    pair = jnp.stack([rows, fetch_band(rows, 1, 0)])
    pairs = [pair] + [fetch_band(pair, 0, d) for d in (1, 2, 3)]
    near, far = [], []
    for z in range(ZH):
        for y in range(NY):
            block = jnp.roll(pairs[y][z], (z, y), axis=(0, 1))
            near.append(jnp.where(c == 0, block[..., :128], block[..., 128:]))
            far.append(jnp.where(c == 0, block[..., 128:], block[..., :128]))
    return [jnp.concatenate(h, axis=-1).reshape(64, 1024) for h in (near, far)]


ARRIVAL = (0, 1, 3, 2)


def by_core(blocks):
    c = position()[2]
    blocks = blocks.reshape(-1, 2, 128, blocks.shape[-1])
    return pick(blocks, c, 1), pick(blocks, 1 - c, 1)


def per_device(orbitals, projectors):
    total_bands = projectors.shape[0] * lax.axis_size("band")
    total_points = projectors.shape[1] * lax.axis_size("grid")
    square = jnp.sum(jnp.square(orbitals.astype(jnp.float32)), axis=1)
    plane, beyond = gather_projectors(projectors)

    states = jnp.concatenate([orbitals, projectors])
    terms = [intersect(plane[y][0], states) for y in ARRIVAL]
    here = reduce_over_x(*by_core(jnp.concatenate(terms)))
    terms = [intersect(rows, states) for y in ARRIVAL for rows in beyond[y]]
    there = reduce_over_x(*by_core(jnp.concatenate(terms)))
    sums = reduce_over_zl(jnp.concatenate([here, there]))
    sums = sums.reshape(ZH, NY, 8, 512)
    sums = jnp.stack([sums[:, ARRIVAL.index(y)] for y in range(NY)], axis=1).reshape(8, 8, 512)
    first, gram = sums[..., :256], sums[..., 256:]
    gram_near, gram_far = gather_gram(gram.astype(jnp.bfloat16).reshape(ZH, NY, 8, 256))

    blocks = [rows for part in (plane, beyond) for y in range(NY) for rows in part[y]]
    near, far = by_core(jnp.concatenate(blocks))
    near, far = near.reshape(1024, -1), far.reshape(1024, -1)

    first_b = first.astype(jnp.bfloat16)
    mine, other = gather_over_grid(first_b)
    mine, other = mine.reshape(1024, 256), other.reshape(1024, 256)
    first, first_b = first.reshape(64, 256), first_b.reshape(64, 256)
    second = first - jnp.dot(gram_near, mine, preferred_element_type=jnp.float32)
    second = second - jnp.dot(gram_far, other, preferred_element_type=jnp.float32)
    second_b = second.astype(jnp.bfloat16)
    value = jnp.sum(second * second_b.astype(jnp.float32), axis=0)
    norm = square - jnp.sum(first_b.astype(jnp.float32) * (first + second), axis=0)

    middle = orbitals.astype(jnp.float32) - apply(mine, near)
    widened = lax.reduce_precision(middle - apply(other, far), 8, 7)

    sums = jnp.stack([*halves(value), *halves(norm)])
    sums = jnp.concatenate([sums, jnp.zeros((4, 256), jnp.bfloat16)])
    rows = jnp.concatenate([second_b.reshape(8, 8, 256), sums[None]])
    mine, other = gather_over_grid(rows)
    sums = sum(h[8, ..., :4, :].astype(jnp.float32).sum(axis=(0, 1)) for h in (mine, other))
    result = widened - apply(mine[:8].reshape(1024, 256), near)
    result = (result - apply(other[:8].reshape(1024, 256), far)).astype(jnp.bfloat16)
    energies = 2.0 * total_points / total_bands * (sums[0] + sums[1]) / (sums[2] + sums[3])
    return (result, energies)


def solution(mesh):
    in_specs = (P("band", "grid"), P("band", "grid"))
    out_specs = (P("band", "grid"), P("band"))
    return jax.shard_map(
        per_device, mesh=mesh, in_specs=in_specs, out_specs=out_specs, check_vma=False
    )
```

```python
import jax
import jax.numpy as jnp
from jax import lax
from jax.sharding import PartitionSpec as P


ZL, NX, NC = 4, 4, 2
ZH, NY = 2, 4


def fetch_band(array, dz, dy):
    pairs = [
        (((z + dz) % ZH) * NY + (y + dy) % NY, z * NY + y)
        for z in range(ZH)
        for y in range(NY)
    ]
    return lax.ppermute(array, "band", pairs)


def grid_pairs(source):
    return [
        (source(zl, x, c), zl * 8 + x * 2 + c)
        for zl in range(ZL)
        for x in range(NX)
        for c in range(NC)
    ]


def from_core(array):
    return lax.ppermute(array, "grid", grid_pairs(lambda zl, x, c: zl * 8 + x * 2 + 1 - c))


def from_x(array, d):
    return lax.ppermute(
        array, "grid", grid_pairs(lambda zl, x, c: zl * 8 + ((x + d) % NX) * 2 + c)
    )


def from_zl(array, d):
    return lax.ppermute(array, "grid", grid_pairs(lambda zl, x, c: (zl ^ d) * 8 + x * 2 + c))


def position():
    g = lax.axis_index("grid")
    return g // 8, (g // 2) % 4, g % 2


def pick(array, at, axis):
    return lax.dynamic_index_in_dim(array, at, axis, keepdims=False)


def reduce_over_x(mine, theirs):
    x = position()[1]
    n, _, cols = mine.shape
    there = from_core(theirs.astype(jnp.bfloat16))
    parts = (mine + there.astype(jnp.float32)).reshape(n, NX, ZL, 8, cols)
    there = []
    for d in (1, 3, 2):
        part = pick(parts, (x + NX - d) % NX, 1).astype(jnp.bfloat16)
        there.append(from_x(part, d))
    return sum((t.astype(jnp.float32) for t in there), pick(parts, x, 1))


def reduce_over_zl(parts):
    zl = position()[0]
    parts = parts.reshape(parts.shape[0], 2, 2, 8, parts.shape[3])
    for d, bit, axis in ((1, zl % 2, 2), (2, zl // 2, 1)):
        there = from_zl(pick(parts, 1 - bit, axis).astype(jnp.bfloat16), d)
        parts = pick(parts, bit, axis) + there.astype(jnp.float32)
    return parts


def placed(pieces, axis):
    length = len(pieces)
    shape = list(pieces[0][1].shape)
    shape.insert(axis, length)
    out = jnp.zeros(shape, pieces[0][1].dtype)
    for at, piece in pieces:
        out = lax.dynamic_update_index_in_dim(out, piece, at, axis)
    return out


def gather_over_grid(rows):
    zl, x, _ = position()
    there = from_zl(rows, 2)
    held = placed([(zl // 2, rows), (1 - zl // 2, there)], 1)
    there = from_zl(held, 1)
    held = placed([(zl % 2, held), (1 - zl % 2, there)], 2)
    held = held.reshape(held.shape[0], ZL, *held.shape[3:])
    there = [((x + d) % NX, from_x(held, d)) for d in (1, 3, 2)]
    held = placed([(x, held)] + there, 1)
    return held, from_core(held)


def intersect(rows, state):
    return lax.dot_general(
        rows, state, (((1,), (1,)), ((), ())), preferred_element_type=jnp.float32
    )


def apply(rounded, rows):
    return lax.dot_general(
        rounded, rows, (((0,), (0,)), ((), ())), preferred_element_type=jnp.float32
    )


def halves(value):
    high = lax.reduce_precision(value, 8, 7)
    return high.astype(jnp.bfloat16), (value - high).astype(jnp.bfloat16)


def gather_projectors(mine):
    up = fetch_band(mine, 0, 1)
    down = fetch_band(mine, 0, 3)
    over = fetch_band(mine, 1, 0)
    up_up = fetch_band(up, 0, 1)
    over_up = fetch_band(over, 0, 1)
    over_down = fetch_band(over, 0, 3)
    last = [fetch_band(over_up[:128], 0, 1), fetch_band(over_down[128:], 0, 3)]
    last = jnp.concatenate(last)
    return [[mine], [up], [up_up], [down]], [[over], [over_up], [last], [over_down]]


def gather_gram(rows):
    c = position()[2]
    pair = jnp.stack([rows, fetch_band(rows, 1, 0)])
    pairs = [pair] + [fetch_band(pair, 0, d) for d in (1, 2, 3)]
    near, far = [], []
    for z in range(ZH):
        for y in range(NY):
            block = jnp.roll(pairs[y][z], (z, y), axis=(0, 1))
            near.append(jnp.where(c == 0, block[..., :128], block[..., 128:]))
            far.append(jnp.where(c == 0, block[..., 128:], block[..., :128]))
    return [jnp.concatenate(h, axis=-1).reshape(64, 1024) for h in (near, far)]


ARRIVAL = (0, 1, 3, 2)


def by_core(blocks):
    c = position()[2]
    blocks = blocks.reshape(-1, 2, 128, blocks.shape[-1])
    return pick(blocks, c, 1), pick(blocks, 1 - c, 1)


def per_device(orbitals, projectors):
    total_bands = projectors.shape[0] * lax.axis_size("band")
    total_points = projectors.shape[1] * lax.axis_size("grid")
    square = jnp.sum(jnp.square(orbitals.astype(jnp.float32)), axis=1)
    plane, beyond = gather_projectors(projectors)

    states = jnp.concatenate([orbitals, projectors])
    terms = [intersect(plane[y][0], states) for y in ARRIVAL]
    here = reduce_over_x(*by_core(jnp.concatenate(terms)))
    terms = [intersect(rows, states) for y in ARRIVAL for rows in beyond[y]]
    there = reduce_over_x(*by_core(jnp.concatenate(terms)))
    sums = reduce_over_zl(jnp.concatenate([here, there]))
    sums = sums.reshape(ZH, NY, 8, 512)
    sums = jnp.stack([sums[:, ARRIVAL.index(y)] for y in range(NY)], axis=1).reshape(8, 8, 512)
    first, gram = sums[..., :256], sums[..., 256:]
    gram_near, gram_far = gather_gram(gram.astype(jnp.bfloat16).reshape(ZH, NY, 8, 256))

    blocks = [rows for part in (plane, beyond) for y in range(NY) for rows in part[y]]
    near, far = by_core(jnp.concatenate(blocks))
    near, far = near.reshape(1024, -1), far.reshape(1024, -1)

    first_b = first.astype(jnp.bfloat16)
    mine, other = gather_over_grid(first_b)
    mine, other = mine.reshape(1024, 256), other.reshape(1024, 256)
    first, first_b = first.reshape(64, 256), first_b.reshape(64, 256)
    second = first - jnp.dot(gram_near, mine, preferred_element_type=jnp.float32)
    second = second - jnp.dot(gram_far, other, preferred_element_type=jnp.float32)
    second_b = second.astype(jnp.bfloat16)
    value = jnp.sum(second * second_b.astype(jnp.float32), axis=0)
    norm = square - jnp.sum(first_b.astype(jnp.float32) * (first + second), axis=0)

    middle = orbitals.astype(jnp.float32) - apply(mine, near)
    widened = lax.reduce_precision(middle - apply(other, far), 8, 7)

    sums = jnp.stack([*halves(value), *halves(norm)])
    sums = jnp.concatenate([sums, jnp.zeros((4, 256), jnp.bfloat16)])
    rows = jnp.concatenate([second_b.reshape(8, 8, 256), sums[None]])
    mine, other = gather_over_grid(rows)
    sums = sum(h[8, ..., :4, :].astype(jnp.float32).sum(axis=(0, 1)) for h in (mine, other))
    result = widened - apply(mine[:8].reshape(1024, 256), near)
    result = (result - apply(other[:8].reshape(1024, 256), far)).astype(jnp.bfloat16)
    energies = 2.0 * total_points / total_bands * (sums[0] + sums[1]) / (sums[2] + sums[3])
    return (result, energies)


def solution(mesh):
    in_specs = (P("band", "grid"), P("band", "grid"))
    out_specs = (P("band", "grid"), P("band"))
    return jax.shard_map(
        per_device, mesh=mesh, in_specs=in_specs, out_specs=out_specs, check_vma=False
    )
```
